32 devices in a mesh: actor: 8 (over z, x), mp: 4 (over y, core).
Axes of the slice: x: 2, y: 2, z: 4, core: 2. Of those that a mesh axis runs over, the one named last changes fastest.
Arguments:
- resid: bfloat16 [8192, 4096], P('actor')
- norm_gain: bfloat16 [4096], replicated, may hold values from 0.25 to 1.75
- query_weight: bfloat16 [4096, 4096], P(None, 'mp'), may hold values from -0.09375 to 0.09375
- cotangent: bfloat16 [8192, 4096], P('actor', 'mp'), may hold values from -0.875 to 0.875
- lengths: int32 [32], P('actor'), may hold values from 1 to 256
- owner: int32 [8], replicated, may hold values from 0 to 7, each once
- adapter_table: float32 [4, 8, 128, 128], P('mp', 'actor')
- moment_one: float32 [4, 8, 128, 128], P('mp', 'actor'), may hold values from -3 to 3
- moment_two: float32 [4, 8, 128, 128], P('mp', 'actor'), may hold values from 0.003 to 0.1
Outputs:
- query: bfloat16 [8192, 4096], P('actor', 'mp')
- adapter_new: float32 [4, 8, 128, 128], P('mp', 'actor')
- moment_one_new: float32 [4, 8, 128, 128], P('mp', 'actor')
- moment_two_new: float32 [4, 8, 128, 128], P('mp', 'actor')
- merged: bfloat16 [4096, 4096], P('actor', 'mp')
The draws below stay inside these ranges and needn't reach their ends.
Inputs may be any that keep to these rules, and one draw needn't show every extreme that they name: owner is a permutation: every actor keeps exactly one block of each feature slice.
All inputs are finite; a program needn't handle non-finite values.
Results may differ from the reference program's by a relative error of at most 0.0064.
Values may be sent and summed in bfloat16 or wider, within the bound.
A program may use at most 128 MiB of HBM per device.

```python
import math
import jax
import jax.numpy as jnp
from jax import lax

D = 4096
R = 64
LEN = 256
TOKENS = 8192
NSEQ = 32
BLK = 128
N_ACTOR = 8
N_MP = 4


def draw_resid(key, part):
    key_base = jax.random.fold_in(key, 11)
    key_rows = jax.random.fold_in(key, 12)
    key_cols = jax.random.fold_in(key, 13)
    rows = jnp.exp(jax.random.uniform(key_rows, (TOKENS, 1), jnp.float32, 0.0, math.log(10.0)))
    cols = jnp.exp(jax.random.uniform(key_cols, (1, D), jnp.float32, 0.0, math.log(10.0)))
    base_output = jax.random.normal(key_base, (TOKENS, D), jnp.float32)
    return (base_output * rows * cols).astype(jnp.bfloat16)


def draw_adapter_table(key, part):
    key_base = jax.random.fold_in(key, 21)
    shape = (N_MP, N_ACTOR, BLK, 2 * R)
    base_output = jax.random.normal(key_base, shape, jnp.float32)
    scales = jnp.concatenate([jnp.full((R,), D ** (-0.5), jnp.float32), jnp.full((R,), R ** (-0.5), jnp.float32)])
    return base_output * scales


def place_ends(array, rng, least, high):
    longest = array.shape.index(max(array.shape))
    spots = []
    for shift in (0, 1):
        where = [jax.random.randint(jax.random.fold_in(rng, axis), (), 0, length) for axis, length in enumerate(array.shape)]
        where[longest] = (where[longest] + shift) % array.shape[longest]
        spots.append(tuple(where))
    return array.at[spots[0]].set(least).at[spots[1]].set(high)


def with_spikes(values, own_key, source, target, shards_of, factor):
    owner, partner = [(jnp.arange(values.shape[dim]) // (values.shape[dim] // shards_of)).reshape([-1 if axis == dim else 1 for axis in range(values.ndim)]) for dim in (source, target)]
    chosen = jax.random.permutation(own_key, shards_of)[partner]
    strong = (owner == chosen) | (owner == (partner + shards_of // 2) % shards_of)
    return jnp.where(strong, factor * values, values)


def block_scale(key, extent, cuts, low, high):
    def one(axis_at, parts):
        steps = jax.random.uniform(jax.random.fold_in(jax.random.fold_in(key, 6), axis_at), (parts,), jnp.float32, low / len(cuts), high / len(cuts))
        return jnp.repeat(jnp.exp(steps), extent[axis_at] // parts).reshape((-1,) + (1,) * (len(extent) - axis_at - 1))

    gain = one(*cuts[0])
    for cut in cuts[1:]:
        gain = gain * one(*cut)
    return gain


def noise(own_key, extent, deviation, reach, shards=(), held_as=jnp.bfloat16):
    factor_of = block_scale(own_key, extent, shards, -0.22, 0.18) if shards else 1.0
    array = jax.random.normal(own_key, extent, jnp.float32) * deviation * factor_of
    return jnp.minimum(jnp.maximum(array, -reach), reach).astype(held_as)


def gaussian_with(stream_key, extent, spread, limit, cuts, heavy, held_as=jnp.bfloat16):
    drawn = spread * jax.random.normal(stream_key, extent, jnp.float32)
    if cuts:
        drawn = drawn * block_scale(stream_key, extent, cuts, -0.22, 0.18)
    return jnp.clip(with_spikes(drawn, jax.random.fold_in(stream_key, 3), *heavy), -limit, limit).astype(held_as)


def setup_inputs(seed: int = 0) -> dict:
    key_list = jax.random.split(jax.random.key(seed), 10)
    return {
        "resid": draw_resid(jax.random.fold_in(key_list[9], 71), 0),
        "norm_gain": jnp.clip(1.0 + 0.15 * jax.random.normal(key_list[1], (D,), jnp.float32), 0.25, 1.75).astype(jnp.bfloat16),
        "query_weight": noise(key_list[2], (D, D), D ** -0.5, 0.09375, ((1, 4),)),
        "cotangent": gaussian_with(key_list[3], (TOKENS, D), 0.1, 0.875, ((0, 8), (1, 4)), (0, 1, 8, 2.0)),
        "lengths": place_ends(jax.random.randint(key_list[4], (NSEQ,), 1, LEN + 1), jax.random.fold_in(key_list[4], 1), 1, LEN).astype(jnp.int32),
        "owner": jax.random.permutation(key_list[5], N_ACTOR).astype(jnp.int32),
        "adapter_table": draw_adapter_table(jax.random.fold_in(key_list[9], 71), 0),
        "moment_one": noise(key_list[7], (N_MP, N_ACTOR, BLK, 2 * R), 0.5, 3.0, ((0, 4), (1, 8)), jnp.float32),
        "moment_two": jnp.clip(jnp.exp(math.log(0.1) - 3.506558 * jax.random.uniform(key_list[8], (N_MP, N_ACTOR, BLK, 2 * R), jnp.float32) ** block_scale(key_list[8], (N_MP, N_ACTOR, BLK, 2 * R), ((0, 4), (1, 8)), -0.2, 0.2)), 0.003, 0.1),
    }


adapter_scale = 0.5
learn_rate = 0.003
beta_one = 0.9
beta_two = 0.999
fix_one = 1.0 - 0.9 ** 10
fix_two = 1.0 - 0.999 ** 10

def build_table(owned, owner):
    ordered = jnp.take(owned, owner, axis=1)
    return ordered.reshape(D, 2 * R)

def reference(resid, norm_gain, query_weight, cotangent, lengths, owner, adapter_table, moment_one, moment_two):
    stream = resid.astype(jnp.float32)
    meansq = lax.optimization_barrier(jnp.mean(stream * stream, axis=1, keepdims=True))
    normalized_input = (stream * lax.rsqrt(meansq + 1e-05) * norm_gain.astype(jnp.float32)[None, :]).astype(jnp.bfloat16)
    index = jnp.arange(TOKENS, dtype=jnp.int32)
    position = index % LEN
    sequence = index // LEN
    active_rows = position < jnp.take(lengths, sequence)
    adapter_now = build_table(adapter_table, owner).astype(jnp.bfloat16)
    mat_a = adapter_now[:, :R]
    mat_bt = adapter_now[:, R:]
    lowrank_output = jnp.dot(normalized_input, mat_a, preferred_element_type=jnp.float32).astype(jnp.bfloat16)
    base_output = jnp.dot(normalized_input, query_weight, preferred_element_type=jnp.float32)
    extra_term = jnp.dot(lowrank_output, mat_bt.T, preferred_element_type=jnp.float32)
    query = jnp.where(active_rows[:, None], base_output + adapter_scale * extra_term, 0.0).astype(jnp.bfloat16)
    masked_rows = jnp.where(active_rows[:, None], cotangent, jnp.zeros_like(cotangent))
    backward_rows = jnp.dot(masked_rows, mat_bt, preferred_element_type=jnp.float32).astype(jnp.bfloat16)
    down_gradient = adapter_scale * jnp.dot(normalized_input.T, backward_rows, preferred_element_type=jnp.float32)
    up_transposed_gradient = adapter_scale * jnp.dot(masked_rows.T, lowrank_output, preferred_element_type=jnp.float32)
    grad = jnp.concatenate([down_gradient, up_transposed_gradient], axis=1)
    grad_blocks = grad.reshape(N_MP, N_ACTOR, BLK, 2 * R)
    grad_owned = jnp.zeros_like(grad_blocks).at[:, owner].set(grad_blocks)
    moment_one_new = beta_one * moment_one + (1.0 - beta_one) * grad_owned
    moment_two_new = beta_two * moment_two + (1.0 - beta_two) * grad_owned * grad_owned
    adapter_new = adapter_table - learn_rate * (moment_one_new / fix_one) / (jnp.sqrt(moment_two_new / fix_two) + 1e-08)
    fresh = build_table(adapter_new, owner).astype(jnp.bfloat16)
    matmul_product = jnp.dot(fresh[:, :R], fresh[:, R:].T, preferred_element_type=jnp.float32)
    merged = (query_weight.astype(jnp.float32) + adapter_scale * matmul_product).astype(jnp.bfloat16)
    return (query, adapter_new, moment_one_new, moment_two_new, merged)
```

```python
import functools

import jax
import jax.numpy as jnp
from jax import lax
from jax.experimental import pallas as pl
from jax.experimental.pallas import tpu as pltpu
from jax.sharding import PartitionSpec as P

MESH = pl.DeviceIdType.MESH
F32 = jnp.float32
BF16 = jnp.bfloat16

adapter_scale = 0.5
learn_rate = 0.003
beta_one = 0.9
beta_two = 0.999
fix_one = 1.0 - 0.9**10
fix_two = 1.0 - 0.999**10

NORM_ROWS = 128
EARLY = 1
MID = 2


def kernel(
    n_actor,
    n_mp,
    lengths,
    owner,
    gain,
    table,
    one,
    two,
    resid,
    weight,
    cotangent,
    query,
    table_new,
    one_new,
    two_new,
    merged,
    x,
    w,
    cot,
    acc,
    qbuf,
    mbuf,
    live,
    gbuf,
    tab,
    pbuf,
    rbuf,
    lb,
    lbr,
    grad,
    sbuf,
    rsbuf,
    nbuf,
    abuf,
    fresh_b,
    fresh_a,
    x_sem,
    w_sem,
    cot_sem,
    q_sem,
    m_sem,
    g_send,
    g_recv,
    p_send,
    p_recv,
    l_send,
    l_recv,
    s_send,
    s_recv,
    n_send,
    n_recv,
    a_send,
    a_recv,
):
    a = lax.axis_index("actor")
    m = lax.axis_index("mp")
    tokens, width = x.shape
    cols = w.shape[1]
    block = table.shape[0]
    lanes = table.shape[1]
    rank = lanes // 2
    nseq = lengths.shape[0]
    seq = tokens // nseq
    part = tokens // n_mp
    share = n_actor // n_mp
    row_count = width // n_actor
    devices = n_actor * n_mp

    norm_steps = tokens // NORM_ROWS

    def x_copy(i):
        rows = pl.ds(pl.multiple_of(i * NORM_ROWS, NORM_ROWS), NORM_ROWS)
        return pltpu.make_async_copy(resid.at[rows], x.at[rows], x_sem.at[i])

    for i in range(norm_steps):
        x_copy(i).start()
    cot_copy = pltpu.make_async_copy(cotangent, cot, cot_sem)
    cot_copy.start()
    w_copy = pltpu.make_async_copy(weight, w, w_sem)
    w_copy.start()

    barrier = pltpu.get_barrier_semaphore()
    me = a * n_mp + m

    @pl.loop(1, devices)
    def _(k):
        other = lax.rem(me + k, devices)
        pl.semaphore_signal(
            barrier, inc=1, device_id=(other // n_mp, lax.rem(other, n_mp)), device_id_type=MESH
        )

    gbuf[0] = table[...].astype(BF16)
    for s in range(nseq):
        live[s * seq : (s + 1) * seq] = jnp.where(
            lax.broadcasted_iota(jnp.int32, (seq, lanes), 0) < lengths[s], 1.0, 0.0
        ).astype(F32)
    pl.semaphore_wait(barrier, devices - 1)

    def to_actor(src, dst, send, recv, k):
        return pltpu.make_async_remote_copy(
            src_ref=src,
            dst_ref=dst,
            send_sem=send.at[k],
            recv_sem=recv.at[k],
            device_id=(lax.rem(a + k, n_actor), m),
            device_id_type=MESH,
        )

    def to_mp(src, dst, send, recv, k):
        return pltpu.make_async_remote_copy(
            src_ref=src,
            dst_ref=dst,
            send_sem=send.at[k],
            recv_sem=recv.at[k],
            device_id=(a, lax.rem(m + k, n_mp)),
            device_id_type=MESH,
        )

    def start_all(copies):
        for copy in copies:
            copy.start()

    def wait_all(copies):
        for copy in copies:
            copy.wait()

    gathers = [to_actor(gbuf.at[0], gbuf.at[k], g_send, g_recv, k) for k in range(1, n_actor)]
    start_all(gathers)

    step = 128

    @pl.loop(0, norm_steps)
    def _(i):
        x_copy(i).wait()
        rows = pl.ds(pl.multiple_of(i * NORM_ROWS, NORM_ROWS), NORM_ROWS)
        total = jnp.zeros((NORM_ROWS, step), F32)
        for c in range(0, width, step):
            v = x[rows, c : c + step].astype(F32)
            total += v * v
        scale = lax.rsqrt(jnp.sum(total, axis=1, keepdims=True) * (1.0 / width) + 1e-05)
        scale = jnp.broadcast_to(scale, (NORM_ROWS, step))
        for c in range(0, width, step):
            v = x[rows, c : c + step].astype(F32)
            g = gain[:, c : c + step].astype(F32)
            x[rows, c : c + step] = (v * scale * g).astype(BF16)

    w_copy.wait()

    def multiply(first, last):
        @pl.loop(first, last)
        def _(i):
            rows = pl.ds(pl.multiple_of(i * seq, seq), seq)
            acc[rows] = jnp.dot(x[rows], w[...], preferred_element_type=F32)

    multiply(0, EARLY)
    cot_copy.wait()
    wait_all(gathers)

    for j in range(n_actor):
        tab[j * block : (j + 1) * block] = gbuf[lax.rem(a - owner[j] + n_actor, n_actor)]

    own_cols = pl.ds(pl.multiple_of(m * cols, cols), cols)

    @pl.loop(0, n_mp)
    def _(q):
        rows = pl.ds(pl.multiple_of(q * part, part), part)
        low_part = jnp.dot(x[rows, own_cols], tab[...], preferred_element_type=F32)
        back_part = jnp.dot(cot[rows], tab[...], preferred_element_type=F32)
        lane = lax.broadcasted_iota(jnp.int32, (part, lanes), 1)
        pbuf[q] = jnp.where(lane < rank, low_part, back_part).astype(BF16)

    sums = [
        to_mp(pbuf.at[lax.rem(m + k, n_mp)], rbuf.at[k], p_send, p_recv, k) for k in range(1, n_mp)
    ]
    start_all(sums)
    multiply(EARLY, MID)
    wait_all(sums)

    mine = pbuf[m].astype(F32)
    for k in range(1, n_mp):
        mine += rbuf[k].astype(F32)
    my_rows = pl.ds(pl.multiple_of(m * part, part), part)
    lb[my_rows] = jnp.where(live[my_rows] > 0.0, mine, 0.0).astype(BF16)
    spreads = [to_mp(lb.at[my_rows], lb.at[my_rows], l_send, l_recv, k) for k in range(1, n_mp)]
    start_all(spreads)
    multiply(MID, nseq)
    wait_all(spreads)

    rolled = pltpu.roll(lb[...].astype(F32), rank, 1)
    lbr[...] = rolled.astype(BF16)
    lbt = rolled.T.astype(BF16)
    down = jnp.dot(lbt, x[:, own_cols], preferred_element_type=F32)
    up = jnp.dot(lbt, cot[...], preferred_element_type=F32)
    row = lax.broadcasted_iota(jnp.int32, (lanes, cols), 0)
    grad[...] = (adapter_scale * jnp.where(row < rank, down, up)).T.reshape(n_actor, block, lanes)

    def position(actor):
        found = jnp.int32(0)
        for j in range(n_actor):
            found = jnp.where(owner[j] == actor, j, found)
        return found

    for k in range(1, n_actor):
        sbuf[k] = grad[position(lax.rem(a + k, n_actor))].astype(BF16)
    scatters = [to_actor(sbuf.at[k], rsbuf.at[k], s_send, s_recv, k) for k in range(1, n_actor)]
    start_all(scatters)

    tab_lane = lax.broadcasted_iota(jnp.int32, (cols, lanes), 1)
    gbuf_b = jnp.where(tab_lane >= rank, tab[...].astype(F32), 0.0).astype(BF16)
    fresh_b[...] = gbuf_b

    def q_copy(i):
        rows = pl.ds(pl.multiple_of(i * seq, seq), seq)
        return pltpu.make_async_copy(qbuf.at[rows], query.at[rows], q_sem.at[i])

    for i in range(nseq):
        rows = pl.ds(i * seq, seq)
        extra = lax.dot_general(
            lbr[rows], fresh_b[...], (((1,), (1,)), ((), ())), preferred_element_type=F32
        )
        alive = lax.broadcasted_iota(jnp.int32, (seq, cols), 0) < lengths[i]
        qbuf[rows] = jnp.where(alive, acc[rows] + adapter_scale * extra, 0.0).astype(BF16)
        q_copy(i).start()

    wait_all(scatters)
    total = grad[position(a)]
    for k in range(1, n_actor):
        total += rsbuf[k].astype(F32)
    first = beta_one * one[...] + (1.0 - beta_one) * total
    second = beta_two * two[...] + (1.0 - beta_two) * total * total
    updated = table[...] - learn_rate * (first / fix_one) / (jnp.sqrt(second / fix_two) + 1e-08)
    nbuf[0] = updated.astype(BF16)

    news = [to_actor(nbuf.at[0], nbuf.at[k], n_send, n_recv, k) for k in range(1, n_actor)]
    downs = []
    for e in range(share):
        target = m * share + e
        slot = lax.rem(target - a + n_actor, n_actor)
        for k in range(1, n_mp):
            downs.append(
                pltpu.make_async_remote_copy(
                    src_ref=nbuf.at[0],
                    dst_ref=abuf.at[slot],
                    send_sem=a_send.at[e * n_mp + k],
                    recv_sem=a_recv.at[slot],
                    device_id=(target, lax.rem(m + k, n_mp)),
                    device_id_type=MESH,
                )
            )
    start_all(news)
    start_all(downs)
    one_new[...] = first
    two_new[...] = second
    table_new[...] = updated

    wait_all(news)
    for copy in downs:
        copy.wait_send()
    source = a // share
    far = source != m

    @pl.when(far)
    def _():
        for k in range(n_actor):
            pltpu.make_async_remote_copy(
                src_ref=nbuf.at[0],
                dst_ref=abuf.at[k],
                send_sem=a_send.at[0],
                recv_sem=a_recv.at[k],
                device_id=(a, lax.rem(m + 1, n_mp)),
                device_id_type=MESH,
            ).wait_recv()

    @pl.when(source == m)
    def _():
        abuf[...] = nbuf[...]

    tail_lane = lax.broadcasted_iota(jnp.int32, (block, lanes), 1)
    for j in range(n_actor):
        block_now = nbuf[lax.rem(a - owner[j] + n_actor, n_actor)].astype(F32)
        turned = pltpu.roll(block_now, rank, 1)
        fresh_b[j * block : (j + 1) * block] = jnp.where(tail_lane < rank, turned, 0.0).astype(BF16)
    start = lax.rem(a, share) * n_mp
    for j in range(n_mp):
        fresh_a[j * block : (j + 1) * block] = abuf[
            lax.rem(a - owner[start + j] + n_actor, n_actor)
        ]
    extra = lax.dot_general(
        fresh_a[...], fresh_b[...], (((1,), (1,)), ((), ())), preferred_element_type=F32
    )
    base = w[pl.ds(pl.multiple_of(a * row_count, row_count), row_count)].astype(F32)
    mbuf[...] = (base + adapter_scale * extra).astype(BF16)
    m_copy = pltpu.make_async_copy(mbuf, merged, m_sem)
    m_copy.start()
    for i in range(nseq):
        q_copy(i).wait()
    m_copy.wait()


def body(
    resid, norm_gain, query_weight, cotangent, lengths, owner, adapter_table, moment_one, moment_two
):
    n_actor = lax.axis_size("actor")
    n_mp = lax.axis_size("mp")
    tokens, width = resid.shape
    cols = query_weight.shape[1]
    block, lanes = adapter_table.shape[2:]
    nseq = lengths.shape[0]
    row_count = width // n_actor
    part = tokens // n_mp
    flat = (block, lanes)
    smem = pl.BlockSpec(memory_space=pltpu.SMEM)
    vmem = pl.BlockSpec(memory_space=pltpu.VMEM)
    hbm = pl.BlockSpec(memory_space=pl.ANY)
    dma = pltpu.SemaphoreType.DMA
    query, updated, first, second, merged = pl.pallas_call(
        functools.partial(kernel, n_actor, n_mp),
        out_shape=(
            jax.ShapeDtypeStruct((tokens, cols), BF16),
            jax.ShapeDtypeStruct(flat, F32),
            jax.ShapeDtypeStruct(flat, F32),
            jax.ShapeDtypeStruct(flat, F32),
            jax.ShapeDtypeStruct((row_count, cols), BF16),
        ),
        in_specs=[smem, smem, vmem, vmem, vmem, vmem, hbm, hbm, hbm],
        out_specs=(hbm, vmem, vmem, vmem, hbm),
        scratch_shapes=[
            pltpu.VMEM((tokens, width), BF16),
            pltpu.VMEM((width, cols), BF16),
            pltpu.VMEM((tokens, cols), BF16),
            pltpu.VMEM((tokens, cols), F32),
            pltpu.VMEM((tokens, cols), BF16),
            pltpu.VMEM((row_count, cols), BF16),
            pltpu.VMEM((tokens, lanes), F32),
            pltpu.VMEM((n_actor, block, lanes), BF16),
            pltpu.VMEM((cols, lanes), BF16),
            pltpu.VMEM((n_mp, part, lanes), BF16),
            pltpu.VMEM((n_mp, part, lanes), BF16),
            pltpu.VMEM((tokens, lanes), BF16),
            pltpu.VMEM((tokens, lanes), BF16),
            pltpu.VMEM((n_actor, block, lanes), F32),
            pltpu.VMEM((n_actor, block, lanes), BF16),
            pltpu.VMEM((n_actor, block, lanes), BF16),
            pltpu.VMEM((n_actor, block, lanes), BF16),
            pltpu.VMEM((n_actor, block, lanes), BF16),
            pltpu.VMEM((cols, lanes), BF16),
            pltpu.VMEM((row_count, lanes), BF16),
            dma((tokens // NORM_ROWS,)),
            dma,
            dma,
            dma((nseq,)),
            dma,
            dma((n_actor,)),
            dma((n_actor,)),
            dma((n_mp,)),
            dma((n_mp,)),
            dma((n_mp,)),
            dma((n_mp,)),
            dma((n_actor,)),
            dma((n_actor,)),
            dma((n_actor,)),
            dma((n_actor,)),
            dma((n_actor,)),
            dma((n_actor,)),
        ],
        compiler_params=pltpu.CompilerParams(
            collective_id=0, has_side_effects=True, vmem_limit_bytes=56 * 2**20
        ),
    )(
        lengths,
        owner,
        norm_gain.reshape(1, width),
        adapter_table.reshape(flat),
        moment_one.reshape(flat),
        moment_two.reshape(flat),
        resid,
        query_weight,
        cotangent,
    )
    shape = adapter_table.shape
    return (query, updated.reshape(shape), first.reshape(shape), second.reshape(shape), merged)


def solution(mesh):
    return jax.shard_map(
        body,
        mesh=mesh,
        in_specs=(
            P("actor", None),
            P(),
            P(None, "mp"),
            P("actor", "mp"),
            P("actor"),
            P(),
            P("mp", "actor", None, None),
            P("mp", "actor", None, None),
            P("mp", "actor", None, None),
        ),
        out_specs=(
            P("actor", "mp"),
            P("mp", "actor", None, None),
            P("mp", "actor", None, None),
            P("mp", "actor", None, None),
            P("actor", "mp"),
        ),
        check_vma=False,
    )
```

```python
import functools

import jax
import jax.numpy as jnp
from jax import lax
from jax.experimental import pallas as pl
from jax.experimental.pallas import tpu as pltpu
from jax.sharding import PartitionSpec as P

MESH = pl.DeviceIdType.MESH
F32 = jnp.float32
BF16 = jnp.bfloat16

adapter_scale = 0.5
learn_rate = 0.003
beta_one = 0.9
beta_two = 0.999
fix_one = 1.0 - 0.9**10
fix_two = 1.0 - 0.999**10

NORM_ROWS = 128
EARLY = 1
MID = 2


def kernel(
    n_actor,
    n_mp,
    lengths,
    owner,
    gain,
    table,
    one,
    two,
    resid,
    weight,
    cotangent,
    query,
    table_new,
    one_new,
    two_new,
    merged,
    x,
    w,
    cot,
    acc,
    live,
    gbuf,
    tab,
    pbuf,
    rbuf,
    lb,
    lbr,
    grad,
    sbuf,
    rsbuf,
    nbuf,
    abuf,
    fresh_b,
    fresh_a,
    gain_row,
    asrc,
    x_sem,
    w_sem,
    cot_sem,
    g_send,
    g_recv,
    p_send,
    p_recv,
    l_send,
    l_recv,
    s_send,
    s_recv,
    n_send,
    n_recv,
    a_send,
    a_recv,
):
    a = lax.axis_index("actor")
    m = lax.axis_index("mp")
    tokens, width = x.shape
    cols = w.shape[1]
    block = table.shape[0]
    lanes = table.shape[1]
    rank = lanes // 2
    nseq = lengths.shape[0]
    seq = tokens // nseq
    part = tokens // n_mp
    share = n_actor // n_mp
    row_count = width // n_actor
    devices = n_actor * n_mp

    norm_steps = tokens // NORM_ROWS

    def x_copy(i):
        rows = pl.ds(pl.multiple_of(i * NORM_ROWS, NORM_ROWS), NORM_ROWS)
        return pltpu.make_async_copy(resid.at[rows], x.at[rows], x_sem.at[i])

    for i in range(norm_steps):
        x_copy(i).start()
    cot_copy = pltpu.make_async_copy(cotangent, cot, cot_sem)
    cot_copy.start()
    w_copy = pltpu.make_async_copy(weight, w, w_sem)
    w_copy.start()

    barrier = pltpu.get_barrier_semaphore()
    me = a * n_mp + m

    @pl.loop(1, devices)
    def _(k):
        other = lax.rem(me + k, devices)
        pl.semaphore_signal(
            barrier, inc=1, device_id=(other // n_mp, lax.rem(other, n_mp)), device_id_type=MESH
        )

    gbuf[0] = table[...].astype(BF16)
    for s in range(nseq):
        live[s * seq : (s + 1) * seq] = jnp.where(
            lax.broadcasted_iota(jnp.int32, (seq, lanes), 0) < lengths[s], 1.0, 0.0
        ).astype(F32)
    pl.semaphore_wait(barrier, devices - 1)

    def to_actor(src, dst, send, recv, k):
        return pltpu.make_async_remote_copy(
            src_ref=src,
            dst_ref=dst,
            send_sem=send.at[k],
            recv_sem=recv.at[k],
            device_id=(lax.rem(a + k, n_actor), m),
            device_id_type=MESH,
        )

    def to_mp(src, dst, send, recv, k):
        return pltpu.make_async_remote_copy(
            src_ref=src,
            dst_ref=dst,
            send_sem=send.at[k],
            recv_sem=recv.at[k],
            device_id=(a, lax.rem(m + k, n_mp)),
            device_id_type=MESH,
        )

    def start_all(copies):
        for copy in copies:
            copy.start()

    def wait_all(copies):
        for copy in copies:
            copy.wait()

    gathers = [to_actor(gbuf.at[0], gbuf.at[k], g_send, g_recv, k) for k in range(1, n_actor)]
    start_all(gathers)

    step = 128
    gain_row[...] = gain[...].astype(F32).reshape(1, width)

    @pl.loop(0, norm_steps)
    def _(i):
        x_copy(i).wait()
        rows = pl.ds(pl.multiple_of(i * NORM_ROWS, NORM_ROWS), NORM_ROWS)
        total = jnp.zeros((NORM_ROWS, step), F32)
        for c in range(0, width, step):
            v = x[rows, c : c + step].astype(F32)
            total += v * v
        scale = lax.rsqrt(jnp.sum(total, axis=1, keepdims=True) * (1.0 / width) + 1e-05)
        scale = jnp.broadcast_to(scale, (NORM_ROWS, step))
        for c in range(0, width, step):
            v = x[rows, c : c + step].astype(F32)
            g = gain_row[:, c : c + step]
            x[rows, c : c + step] = (v * scale * g).astype(BF16)

    w_copy.wait()

    def multiply(first, last):
        @pl.loop(first, last)
        def _(i):
            rows = pl.ds(pl.multiple_of(i * seq, seq), seq)
            acc[rows] = jnp.dot(x[rows], w[...], preferred_element_type=F32)

    multiply(0, EARLY)
    cot_copy.wait()
    wait_all(gathers)

    for j in range(n_actor):
        tab[j * block : (j + 1) * block] = gbuf[lax.rem(a - owner[j] + n_actor, n_actor)]

    own_cols = pl.ds(pl.multiple_of(m * cols, cols), cols)

    @pl.loop(0, n_mp)
    def _(q):
        rows = pl.ds(pl.multiple_of(q * part, part), part)
        low_part = jnp.dot(x[rows, own_cols], tab[...], preferred_element_type=F32)
        back_part = jnp.dot(cot[rows], tab[...], preferred_element_type=F32)
        lane = lax.broadcasted_iota(jnp.int32, (part, lanes), 1)
        pbuf[q] = jnp.where(lane < rank, low_part, back_part).astype(BF16)

    sums = [
        to_mp(pbuf.at[lax.rem(m + k, n_mp)], rbuf.at[k], p_send, p_recv, k) for k in range(1, n_mp)
    ]
    start_all(sums)
    multiply(EARLY, MID)
    wait_all(sums)

    mine = pbuf[m].astype(F32)
    for k in range(1, n_mp):
        mine += rbuf[k].astype(F32)
    my_rows = pl.ds(pl.multiple_of(m * part, part), part)
    lb[my_rows] = jnp.where(live[my_rows] > 0.0, mine, 0.0).astype(BF16)
    spreads = [to_mp(lb.at[my_rows], lb.at[my_rows], l_send, l_recv, k) for k in range(1, n_mp)]
    start_all(spreads)
    multiply(MID, nseq)
    wait_all(spreads)

    rolled = pltpu.roll(lb[...].astype(F32), rank, 1)
    lbr[...] = rolled.astype(BF16)
    lbt = rolled.T.astype(BF16)
    down = jnp.dot(lbt, x[:, own_cols], preferred_element_type=F32)
    up = jnp.dot(lbt, cot[...], preferred_element_type=F32)
    row = lax.broadcasted_iota(jnp.int32, (lanes, cols), 0)
    grad[...] = (adapter_scale * jnp.where(row < rank, down, up)).T.reshape(n_actor, block, lanes)

    def position(actor):
        found = jnp.int32(0)
        for j in range(n_actor):
            found = jnp.where(owner[j] == actor, j, found)
        return found

    for k in range(1, n_actor):
        sbuf[k] = grad[position(lax.rem(a + k, n_actor))].astype(BF16)
    scatters = [to_actor(sbuf.at[k], rsbuf.at[k], s_send, s_recv, k) for k in range(1, n_actor)]
    start_all(scatters)

    tab_lane = lax.broadcasted_iota(jnp.int32, (cols, lanes), 1)
    gbuf_b = jnp.where(tab_lane >= rank, tab[...].astype(F32), 0.0).astype(BF16)
    fresh_b[...] = gbuf_b

    for i in range(nseq):
        rows = pl.ds(i * seq, seq)
        extra = lax.dot_general(
            lbr[rows], fresh_b[...], (((1,), (1,)), ((), ())), preferred_element_type=F32
        )
        alive = lax.broadcasted_iota(jnp.int32, (seq, cols), 0) < lengths[i]
        query[rows] = jnp.where(alive, acc[rows] + adapter_scale * extra, 0.0).astype(BF16)

    wait_all(scatters)
    total = grad[position(a)]
    for k in range(1, n_actor):
        total += rsbuf[k].astype(F32)
    first = beta_one * one[...] + (1.0 - beta_one) * total
    second = beta_two * two[...] + (1.0 - beta_two) * total * total
    updated = table[...] - learn_rate * (first / fix_one) / (jnp.sqrt(second / fix_two) + 1e-08)
    half = block // 2
    top, bottom = updated[:half], updated[half:]
    left = lax.broadcasted_iota(jnp.int32, (half, lanes), 1) < rank
    asrc[...] = jnp.where(left, top, pltpu.roll(bottom, rank, 1)).astype(BF16)
    nbuf[0] = jnp.where(left, pltpu.roll(top, rank, 1), bottom).astype(BF16)

    source = a // share

    def down(e, k):
        target = m * share + e
        slot = lax.rem(target - a + n_actor, n_actor)
        return pltpu.make_async_remote_copy(
            src_ref=asrc,
            dst_ref=abuf.at[slot],
            send_sem=a_send.at[e * n_mp + k],
            recv_sem=a_recv.at[slot],
            device_id=(target, lax.rem(m + k, n_mp)),
            device_id_type=MESH,
        )

    news = [to_actor(nbuf.at[0], nbuf.at[k], n_send, n_recv, k) for k in range(1, n_actor)]
    for e in range(share):
        for k in range(1, n_mp):
            down(e, k).start()

        @pl.when(m * share + e != a)
        def _():
            down(e, 0).start()

    start_all(news)

    @pl.when(source == m)
    def _():
        abuf[0] = asrc[...]

    one_new[...] = first
    two_new[...] = second
    table_new[...] = updated

    def arrived(k):
        pltpu.make_async_remote_copy(
            src_ref=asrc,
            dst_ref=abuf.at[k],
            send_sem=a_send.at[0],
            recv_sem=a_recv.at[k],
            device_id=(a, lax.rem(m + 1, n_mp)),
            device_id_type=MESH,
        ).wait_recv()

    for k in range(1, n_actor):
        arrived(k)

    @pl.when(source != m)
    def _():
        arrived(0)

    wait_all(news)
    for e in range(share):
        for k in range(1, n_mp):
            down(e, k).wait_send()

        @pl.when(m * share + e != a)
        def _():
            down(e, 0).wait_send()

    for j in range(n_actor):
        packed = nbuf[lax.rem(a - owner[j] + n_actor, n_actor)].astype(F32)
        rows = j * block
        fresh_b[rows : rows + half] = jnp.where(left, packed, 0.0).astype(BF16)
        fresh_b[rows + half : rows + block] = jnp.where(
            left, pltpu.roll(packed, rank, 1), 0.0
        ).astype(BF16)
    start = lax.rem(a, share) * n_mp
    for j in range(n_mp):
        packed = abuf[lax.rem(a - owner[start + j] + n_actor, n_actor)].astype(F32)
        rows = j * block
        fresh_a[rows : rows + half] = packed.astype(BF16)
        fresh_a[rows + half : rows + block] = pltpu.roll(packed, rank, 1).astype(BF16)
    extra = lax.dot_general(
        fresh_a[...], fresh_b[...], (((1,), (1,)), ((), ())), preferred_element_type=F32
    )
    base = w[pl.ds(pl.multiple_of(a * row_count, row_count), row_count)].astype(F32)
    merged[...] = (base + adapter_scale * extra).astype(BF16)


def put_out(*refs):
    count = len(refs) // 2
    sems = refs[-1]
    copies = [
        pltpu.make_async_copy(refs[i], refs[count + i], sems.at[i]) for i in range(count)
    ]
    for copy in copies:
        copy.start()
    for copy in copies:
        copy.wait()


def body(
    resid, norm_gain, query_weight, cotangent, lengths, owner, adapter_table, moment_one, moment_two
):
    n_actor = lax.axis_size("actor")
    n_mp = lax.axis_size("mp")
    tokens, width = resid.shape
    cols = query_weight.shape[1]
    block, lanes = adapter_table.shape[2:]
    nseq = lengths.shape[0]
    row_count = width // n_actor
    part = tokens // n_mp
    flat = (block, lanes)
    smem = pl.BlockSpec(memory_space=pltpu.SMEM)
    vmem = pl.BlockSpec(memory_space=pltpu.VMEM)
    hbm = pl.BlockSpec(memory_space=pl.ANY)
    dma = pltpu.SemaphoreType.DMA
    shapes = (
        ((tokens, cols), BF16),
        (flat, F32),
        (flat, F32),
        (flat, F32),
        ((row_count, cols), BF16),
    )
    results = pl.pallas_call(
        functools.partial(kernel, n_actor, n_mp),
        out_shape=tuple(pltpu.VMEM(shape, dtype) for shape, dtype in shapes),
        in_specs=[smem, smem, vmem, vmem, vmem, vmem, hbm, hbm, hbm],
        out_specs=(vmem,) * len(shapes),
        scratch_shapes=[
            pltpu.VMEM((tokens, width), BF16),
            pltpu.VMEM((width, cols), BF16),
            pltpu.VMEM((tokens, cols), BF16),
            pltpu.VMEM((tokens, cols), F32),
            pltpu.VMEM((tokens, lanes), F32),
            pltpu.VMEM((n_actor, block, lanes), BF16),
            pltpu.VMEM((cols, lanes), BF16),
            pltpu.VMEM((n_mp, part, lanes), BF16),
            pltpu.VMEM((n_mp, part, lanes), BF16),
            pltpu.VMEM((tokens, lanes), BF16),
            pltpu.VMEM((tokens, lanes), BF16),
            pltpu.VMEM((n_actor, block, lanes), F32),
            pltpu.VMEM((n_actor, block, lanes), BF16),
            pltpu.VMEM((n_actor, block, lanes), BF16),
            pltpu.VMEM((n_actor, block // 2, lanes), BF16),
            pltpu.VMEM((n_actor, block // 2, lanes), BF16),
            pltpu.VMEM((cols, lanes), BF16),
            pltpu.VMEM((row_count, lanes), BF16),
            pltpu.VMEM((1, width), F32),
            pltpu.VMEM((block // 2, lanes), BF16),
            dma((tokens // NORM_ROWS,)),
            dma,
            dma,
            dma((n_actor,)),
            dma((n_actor,)),
            dma((n_mp,)),
            dma((n_mp,)),
            dma((n_mp,)),
            dma((n_mp,)),
            dma((n_actor,)),
            dma((n_actor,)),
            dma((n_actor,)),
            dma((n_actor,)),
            dma((n_actor,)),
            dma((n_actor,)),
        ],
        compiler_params=pltpu.CompilerParams(
            collective_id=0, has_side_effects=True, vmem_limit_bytes=56 * 2**20
        ),
    )(
        lengths,
        owner,
        norm_gain,
        adapter_table.reshape(flat),
        moment_one.reshape(flat),
        moment_two.reshape(flat),
        resid,
        query_weight,
        cotangent,
    )
    query, updated, first, second, merged = pl.pallas_call(
        put_out,
        out_shape=tuple(jax.ShapeDtypeStruct(shape, dtype) for shape, dtype in shapes),
        in_specs=[vmem] * len(shapes),
        out_specs=(hbm,) * len(shapes),
        scratch_shapes=[dma((len(shapes),))],
        compiler_params=pltpu.CompilerParams(vmem_limit_bytes=2**20),
    )(*results)
    shape = adapter_table.shape
    return (query, updated.reshape(shape), first.reshape(shape), second.reshape(shape), merged)


def solution(mesh):
    return jax.shard_map(
        body,
        mesh=mesh,
        in_specs=(
            P("actor", None),
            P(),
            P(None, "mp"),
            P("actor", "mp"),
            P("actor"),
            P(),
            P("mp", "actor", None, None),
            P("mp", "actor", None, None),
            P("mp", "actor", None, None),
        ),
        out_specs=(
            P("actor", "mp"),
            P("mp", "actor", None, None),
            P("mp", "actor", None, None),
            P("mp", "actor", None, None),
            P("actor", "mp"),
        ),
        check_vma=False,
    )
```
